32 devices in a mesh: row: 8 (over z, x), col: 4 (over y, core).
Axes of the slice: x: 2, y: 2, z: 4, core: 2. Of those that a mesh axis runs over, the one named last changes fastest.
Arguments:
- source_points: bfloat16 [512, 64, 128], P(('row', 'col')), may hold values from -1.5 to 1.5
- target_points: bfloat16 [512, 64, 128], P(('row', 'col')), may hold values from -1.5 to 1.5
- source_mass: float32 [512, 128], P(('row', 'col')), may hold values from -4 to 4
- target_mass: float32 [512, 128], P(('row', 'col')), may hold values from -4 to 4
- support: int32 [512, 32], P(('row', 'col')), may hold values from 0 to 511, as said below
- coarse_potential: float32 [512, 128], P(('row', 'col')), may hold values from -4 to 150
Outputs:
- potential_f: float32 [512, 128], P(('row', 'col'))
- potential_g: float32 [512, 128], P(('row', 'col'))
The draws below stay inside these ranges and needn't reach their ends.
Inputs may be any that keep to these rules, and one draw needn't show every extreme that they name: `support`: each row names 32 different target clusters. The rows of one device's 16 source clusters name, among the 16 target clusters of any one device, exactly 2 different ones. Every target cluster is named by some row.
All inputs are finite; a program needn't handle non-finite values.
Results may differ from the reference program's by a relative error of at most 0.0003.
Values may be sent and summed in bfloat16 or wider, within the bound.
A program may use at most 64 MiB of HBM per device.

```python
import jax
import jax.numpy as jnp
from jax import lax

D = 64
PTS = 128
SUP = 32
CAP = 2
ITERS = 2
CL_DEV = 16
SRC_CL = 512
TGT_CL = 512
DEVICES = 32


def shuffle(subkey):
    return jax.random.permutation(subkey, DEVICES * CAP)


def pick_some(subkey):
    return jax.random.permutation(subkey, DEVICES * CAP)[:SUP]


def reorder(subkey):
    return jax.random.permutation(subkey, CL_DEV)


def draw_support(key, part):
    listed = DEVICES * CAP
    covering = -(-listed // SUP)
    offsets = jax.random.randint(jax.random.fold_in(key, 11), (DEVICES,), 0, CL_DEV)
    subkeys = jax.random.split(jax.random.fold_in(key, 12), DEVICES)
    orders = jax.vmap(shuffle)(subkeys)
    owners = orders // CAP
    within = orders % CAP
    requester = jnp.arange(DEVICES)[:, None]
    local = (requester * CAP + within + offsets[owners]) % CL_DEV
    entries = owners * CL_DEV + local
    row_ids = jnp.arange(CL_DEV)
    periodic = (row_ids[:, None] * SUP + jnp.arange(SUP)[None, :]) % listed
    row_keys = jax.random.split(jax.random.fold_in(key, 13), DEVICES * CL_DEV)
    scattered = jax.vmap(pick_some)(row_keys).reshape(DEVICES, CL_DEV, SUP)
    position = jnp.where(row_ids[None, :, None] < covering, periodic[None, :, :], scattered)
    row_orders = jax.vmap(reorder)(jax.random.split(jax.random.fold_in(key, 14), DEVICES))
    position = jnp.take_along_axis(position, row_orders[:, :, None], axis=1)
    chosen = jnp.take_along_axis(entries, position.reshape(DEVICES, CL_DEV * SUP), axis=1)
    return chosen.reshape(DEVICES * CL_DEV, SUP).astype(jnp.int32)


def feature_signs(key):
    flips = jax.random.randint(jax.random.fold_in(key, 31), (D,), 0, 2)
    return (2 * flips - 1).astype(jnp.float32)


def draw_embedded(key, salt):
    shape = (CL_DEV * DEVICES, D, PTS)
    offset = 0.6 * feature_signs(key)[None, :, None]
    noise = 0.25 * jax.random.normal(jax.random.fold_in(key, salt), shape, jnp.float32)
    return jnp.clip(noise + offset, -1.5, 1.5).astype(jnp.bfloat16)


def draw_source_points(key, part):
    return draw_embedded(key, 41)


def draw_target_points(key, part):
    return draw_embedded(key, 42)


def draw_coarse_potential(key, part):
    shape = (CL_DEV * DEVICES, PTS)
    return jnp.clip(jax.random.normal(jax.random.fold_in(key, 24), shape, jnp.float32), -4.0, 4.0)


def block_levels(rng, shape, cuts, low, largest):
    gain, own = 1.0, jax.random.fold_in(rng, 6)
    for dim, blocks in cuts:
        heights = jnp.exp(jax.random.uniform(jax.random.fold_in(own, dim), (blocks,), jnp.float32, low / len(cuts), largest / len(cuts)))
        gain = gain * jnp.repeat(heights, shape[dim] // blocks).reshape([-1 if axis == dim else 1 for axis in range(len(shape))])
    return gain


def centred(key, shape, width, limit, pieces=(), held_as=jnp.bfloat16):
    level = block_levels(key, shape, pieces, -0.22, 0.18) if pieces else 1.0
    array = jax.random.normal(key, shape, jnp.float32) * width * level
    return jnp.minimum(jnp.maximum(array, -limit), limit).astype(held_as)


def setup_inputs(seed: int = 0) -> dict:
    keys = jax.random.split(jax.random.key(seed), 7)
    source_points = draw_source_points(jax.random.fold_in(keys[6], 71), 0)
    target_points = draw_target_points(jax.random.fold_in(keys[6], 71), 0)
    source_mass = centred(keys[2], (SRC_CL, PTS), 1.0, 4.0, ((0, 32),), jnp.float32)
    target_mass = centred(keys[3], (TGT_CL, PTS), 1.0, 4.0, ((0, 32),), jnp.float32)
    support = draw_support(jax.random.fold_in(keys[6], 71), 0)
    coarse_potential = draw_coarse_potential(jax.random.fold_in(keys[6], 71), 0)
    return dict(source_points=source_points, target_points=target_points, source_mass=source_mass, target_mass=target_mass, support=support, coarse_potential=coarse_potential)


epsilon = 0.5
lowest = -1e30


def squares(points):
    wide = points.astype(jnp.float32)
    return jnp.sum(wide * wide, axis=-2)


def cluster_terms(source, source_sq, source_log, tiles, tiles_sq, shifted):
    cross = jnp.einsum("dp,tdq->tpq", source.astype(jnp.float32), tiles.astype(jnp.float32))
    cost = source_sq[None, :, None] + tiles_sq[:, None, :] - 2.0 * cross
    scores = (shifted[:, None, :] - cost) / epsilon
    peak = jnp.max(scores, axis=(0, 2))
    total = jnp.sum(jnp.exp(scores - peak[None, :, None]), axis=(0, 2))
    potential = -epsilon * (peak + jnp.log(total))
    lifted = potential + epsilon * source_log
    backward = (lifted[None, :, None] - cost) / epsilon
    column_peak = jnp.max(backward, axis=1)
    column_total = jnp.sum(jnp.exp(backward - column_peak[:, None, :]), axis=1)
    return potential, column_peak, column_total


def fold_max(old_max, old_sum, new_max, new_sum):
    upper = jnp.maximum(old_max, new_max)
    return upper, old_sum * jnp.exp(old_max - upper) + new_sum * jnp.exp(new_max - upper)


def reference(source_points, target_points, source_mass, target_mass, support, coarse_potential):
    source_sq = squares(source_points)
    target_sq = squares(target_points)
    potential_g = coarse_potential
    potential_f = jnp.zeros(source_mass.shape, jnp.float32)
    for sweep in range(ITERS):
        shifted_all = potential_g + epsilon * target_mass

        def visit(carry, item):
            run_max, run_sum = carry
            source, sq_row, log_row, targets = item
            potential, column_peak, column_total = cluster_terms(
                source, sq_row, log_row, target_points[targets], target_sq[targets], shifted_all[targets])
            upper, summed = fold_max(run_max[targets], run_sum[targets], column_peak, column_total)
            return (run_max.at[targets].set(upper), run_sum.at[targets].set(summed)), potential

        start = (jnp.full(coarse_potential.shape, lowest, jnp.float32), jnp.zeros(coarse_potential.shape, jnp.float32))
        (run_max, run_sum), potential_f = lax.scan(visit, start, (source_points, source_sq, source_mass, support))
        potential_g = -epsilon * (run_max + jnp.log(run_sum))
    return potential_f, potential_g
```

```python
import jax
import jax.numpy as jnp
from jax import lax
from jax.experimental import pallas as pl
from jax.experimental.pallas import tpu as pltpu
from jax.sharding import PartitionSpec as P

CAP = 2
ITERS = 2
AXES = ("row", "col")
GROUP = 4


epsilon = 0.5
lowest = -1e30


def squares(points):
    wide = points.astype(jnp.float32)
    return jnp.sum(wide * wide, axis=-2)


def pieces(row, depth):
    high = row.astype(jnp.bfloat16).astype(jnp.float32)
    rest = row - high
    middle = rest.astype(jnp.bfloat16).astype(jnp.float32)
    low = rest - middle
    index = lax.broadcasted_iota(jnp.int32, (depth, row.shape[1]), 0)
    return jnp.where(
        index == 0, high, jnp.where(index == 1, middle, jnp.where(index == 2, low, 0.0))
    )


def ones_rows(depth, points):
    index = lax.broadcasted_iota(jnp.int32, (depth, points), 0)
    return jnp.where(index < 3, 1.0, 0.0)


def fold(old_max, old_sum, scores):
    rows, lanes = scores.shape
    blocks = scores.reshape(rows // 8, 8, lanes)
    upper = jnp.maximum(old_max, jnp.max(blocks, axis=0))
    total = old_sum * jnp.exp(old_max - upper) + jnp.sum(jnp.exp(blocks - upper[None]), axis=0)
    return upper, total


def sweep_kernel(
    slots_ref, source_ref, mass_ref, tiles_ref, u_ref, row_ref, column_ref,
    tile_forward, tile_backward, run_max, run_sum,
):
    clusters, features, points = source_ref.shape
    slots = tiles_ref.shape[0]
    entries = slots_ref.shape[1]
    spare = tile_forward.shape[2] - features
    ones = ones_rows(spare, points)

    def prepare(slot, carry):
        tile = tiles_ref[slot].astype(jnp.float32)
        extra = pieces(u_ref[pl.ds(slot, 1), :], spare)
        tile_forward[slot] = jnp.concatenate([4.0 * tile, extra], axis=0).T.astype(jnp.bfloat16)
        tile_backward[slot] = jnp.concatenate([tile, ones], axis=0).astype(jnp.bfloat16)
        run_max[slot] = jnp.full((8, points), lowest, jnp.float32)
        run_sum[slot] = jnp.zeros((8, points), jnp.float32)
        return carry

    lax.fori_loop(0, slots, prepare, 0, unroll=4)

    def visit(cluster, carry):
        source = source_ref[cluster].astype(jnp.float32)
        right = jnp.concatenate([source, ones], axis=0).astype(jnp.bfloat16)

        def forward(step, state):
            lhs = jnp.concatenate(
                [tile_forward[slots_ref[cluster, step * GROUP + lane]] for lane in range(GROUP)],
                axis=0,
            )
            return fold(*state, jnp.dot(lhs, right, preferred_element_type=jnp.float32))

        start = (
            jnp.full((8, points), lowest, jnp.float32),
            jnp.zeros((8, points), jnp.float32),
        )
        upper, total = lax.fori_loop(0, entries // GROUP, forward, start, unroll=True)
        peak = jnp.max(upper, axis=0, keepdims=True)
        total = jnp.sum(total * jnp.exp(upper - peak), axis=0, keepdims=True)
        level = peak + jnp.log(total)
        row_ref[pl.ds(cluster, 1), :] = level
        extra = pieces(mass_ref[pl.ds(cluster, 1), :] - level, spare)
        left = jnp.concatenate([4.0 * source, extra], axis=0).T.astype(jnp.bfloat16)

        def backward(step, state):
            chosen = [slots_ref[cluster, step * GROUP + lane] for lane in range(GROUP)]
            held = [(run_max[slot], run_sum[slot]) for slot in chosen]
            rhs = jnp.concatenate([tile_backward[slot] for slot in chosen], axis=1)
            scores = jnp.dot(left, rhs, preferred_element_type=jnp.float32)
            fresh = [
                fold(*held[lane], scores[:, lane * points : (lane + 1) * points])
                for lane in range(GROUP)
            ]
            for slot, (new_max, new_sum) in zip(chosen, fresh):
                run_max[slot] = new_max
                run_sum[slot] = new_sum
            return state

        lax.fori_loop(0, entries // GROUP, backward, 0, unroll=True)
        return carry

    lax.fori_loop(0, clusters, visit, 0)
    upper = run_max[...]
    peak = jnp.max(upper, axis=1, keepdims=True)
    total = jnp.sum(run_sum[...] * jnp.exp(upper - peak), axis=1)
    column_ref[...] = peak[:, 0] + jnp.log(total)


def sweep_call(slot_list, source, mass, tiles, u):
    clusters, features, points = source.shape
    slots = tiles.shape[0]
    depth = 2 * features
    vmem = pl.BlockSpec(memory_space=pltpu.VMEM)
    pairs = clusters * slot_list.shape[1]
    return pl.pallas_call(
        sweep_kernel,
        out_shape=(
            jax.ShapeDtypeStruct((clusters, points), jnp.float32),
            jax.ShapeDtypeStruct((slots, points), jnp.float32),
        ),
        in_specs=[pl.BlockSpec(memory_space=pltpu.SMEM), vmem, vmem, vmem, vmem],
        out_specs=(vmem, vmem),
        scratch_shapes=[
            pltpu.VMEM((slots, points, depth), jnp.bfloat16),
            pltpu.VMEM((slots, depth, points), jnp.bfloat16),
            pltpu.VMEM((slots, 8, points), jnp.float32),
            pltpu.VMEM((slots, 8, points), jnp.float32),
        ],
        cost_estimate=pl.CostEstimate(
            flops=4 * pairs * points * points * depth,
            transcendentals=2 * pairs * points * points,
            bytes_accessed=2 * slots * features * points,
        ),
        name="sweep",
    )(slot_list, source, mass, tiles, u)


def exchange(array):
    return lax.all_to_all(array, AXES, split_axis=0, concat_axis=0, tiled=True)


def body(source_points, target_points, source_mass, target_mass, support, coarse_potential):
    devices = lax.axis_size(AXES)
    local_count, features, points = source_points.shape
    owner = support // local_count
    within = support % local_count
    flat_owner, flat_within = owner.reshape(-1), within.reshape(-1)
    named = flat_owner[None, :] == jnp.arange(devices, dtype=jnp.int32)[:, None]
    first = jnp.min(jnp.where(named, flat_within[None, :], local_count), axis=1)
    second = jnp.max(jnp.where(named, flat_within[None, :], -1), axis=1)
    request = jnp.stack([first, second], axis=1)
    first_of = jnp.sum(jnp.where(named, first[:, None], 0), axis=0).reshape(owner.shape)
    slot_list = (owner * CAP + (within > first_of).astype(jnp.int32)).astype(jnp.int32)
    asked = exchange(request)

    target_sq = squares(target_points)
    source_sq = squares(source_points)
    u = 2.0 * (coarse_potential - target_sq) + target_mass
    tiles = exchange(target_points[asked]).reshape(devices * CAP, features, points)
    flat_asked = asked.reshape(-1)
    matches = flat_asked[:, None] == jnp.arange(local_count, dtype=jnp.int32)[None, :]
    for sweep in range(ITERS):
        sending = jnp.sum(jnp.where(matches[:, :, None], u[None, :, :], 0.0), axis=1)
        received = exchange(sending.reshape(devices, CAP, points)).reshape(devices * CAP, points)
        level, column = sweep_call(slot_list, source_points, source_mass, tiles, received)
        peer = exchange(column.reshape(devices, CAP, points)).reshape(devices * CAP, points)
        masked = jnp.where(matches[:, :, None], peer[:, None, :], lowest)
        upper = jnp.max(masked, axis=0)
        total = jnp.sum(jnp.exp(masked - upper[None]), axis=0)
        column_level = upper + jnp.log(total)
        u = target_mass - column_level
    return (source_sq - 0.5 * level, target_sq - 0.5 * column_level)


def solution(mesh):
    placed = (
        P(AXES, None, None),
        P(AXES, None, None),
        P(AXES, None),
        P(AXES, None),
        P(AXES, None),
        P(AXES, None),
    )
    return jax.shard_map(
        body,
        mesh=mesh,
        in_specs=placed,
        out_specs=(P(AXES, None), P(AXES, None)),
        check_vma=False,
    )
```

```python
import functools

import jax
import jax.numpy as jnp
from jax import lax
from jax.experimental import pallas as pl
from jax.experimental.pallas import tpu as pltpu
from jax.sharding import PartitionSpec as P

CAP = 2
ITERS = 2
AXES = ("row", "col")
GROUP = 4
MESH = pl.DeviceIdType.MESH


epsilon = 0.5
lowest = -1e30


def squares(points):
    wide = points.astype(jnp.float32)
    return jnp.sum(wide * wide, axis=-2)


def pieces(row, depth):
    high = row.astype(jnp.bfloat16).astype(jnp.float32)
    rest = row - high
    middle = rest.astype(jnp.bfloat16).astype(jnp.float32)
    low = rest - middle
    index = lax.broadcasted_iota(jnp.int32, (depth, row.shape[1]), 0)
    return jnp.where(
        index == 0, high, jnp.where(index == 1, middle, jnp.where(index == 2, low, 0.0))
    )


def ones_rows(depth, points):
    index = lax.broadcasted_iota(jnp.int32, (depth, points), 0)
    return jnp.where(index < 3, 1.0, 0.0)


def fold(old_max, old_sum, scores):
    rows, lanes = scores.shape
    blocks = scores.reshape(rows // 8, 8, lanes)
    upper = jnp.maximum(old_max, jnp.max(blocks, axis=0))
    total = old_sum * jnp.exp(old_max - upper) + jnp.sum(jnp.exp(blocks - upper[None]), axis=0)
    return upper, total


def sweep_kernel(
    slots_ref, source_ref, mass_ref, tiles_ref, u_ref, row_ref, column_ref,
    tile_forward, tile_backward, run_max, run_sum,
):
    clusters, features, points = source_ref.shape
    slots = tiles_ref.shape[0]
    entries = slots_ref.shape[1]
    spare = tile_forward.shape[2] - features
    ones = ones_rows(spare, points)

    def prepare(slot, carry):
        tile = tiles_ref[slot].astype(jnp.float32)
        extra = pieces(u_ref[pl.ds(slot, 1), :], spare)
        tile_forward[slot] = jnp.concatenate([4.0 * tile, extra], axis=0).T.astype(jnp.bfloat16)
        tile_backward[slot] = jnp.concatenate([tile, ones], axis=0).astype(jnp.bfloat16)
        run_max[slot] = jnp.full((8, points), lowest, jnp.float32)
        run_sum[slot] = jnp.zeros((8, points), jnp.float32)
        return carry

    lax.fori_loop(0, slots, prepare, 0, unroll=4)

    def visit(cluster, carry):
        source = source_ref[cluster].astype(jnp.float32)
        right = jnp.concatenate([source, ones], axis=0).astype(jnp.bfloat16)

        def forward(step, state):
            lhs = jnp.concatenate(
                [tile_forward[slots_ref[cluster, step * GROUP + lane]] for lane in range(GROUP)],
                axis=0,
            )
            return fold(*state, jnp.dot(lhs, right, preferred_element_type=jnp.float32))

        start = (
            jnp.full((8, points), lowest, jnp.float32),
            jnp.zeros((8, points), jnp.float32),
        )
        upper, total = lax.fori_loop(0, entries // GROUP, forward, start, unroll=True)
        peak = jnp.max(upper, axis=0, keepdims=True)
        total = jnp.sum(total * jnp.exp(upper - peak), axis=0, keepdims=True)
        level = peak + jnp.log(total)
        row_ref[pl.ds(cluster, 1), :] = level
        extra = pieces(mass_ref[pl.ds(cluster, 1), :] - level, spare)
        left = jnp.concatenate([4.0 * source, extra], axis=0).T.astype(jnp.bfloat16)

        def backward(step, state):
            chosen = [slots_ref[cluster, step * GROUP + lane] for lane in range(GROUP)]
            held = [(run_max[slot], run_sum[slot]) for slot in chosen]
            rhs = jnp.concatenate([tile_backward[slot] for slot in chosen], axis=1)
            scores = jnp.dot(left, rhs, preferred_element_type=jnp.float32)
            fresh = [
                fold(*held[lane], scores[:, lane * points : (lane + 1) * points])
                for lane in range(GROUP)
            ]
            for slot, (new_max, new_sum) in zip(chosen, fresh):
                run_max[slot] = new_max
                run_sum[slot] = new_sum
            return state

        lax.fori_loop(0, entries // GROUP, backward, 0, unroll=True)
        return carry

    lax.fori_loop(0, clusters, visit, 0)
    upper = run_max[...]
    peak = jnp.max(upper, axis=1, keepdims=True)
    total = jnp.sum(run_sum[...] * jnp.exp(upper - peak), axis=1)
    column_ref[...] = peak[:, 0] + jnp.log(total)


def sweep_call(slot_list, source, mass, tiles, u):
    clusters, features, points = source.shape
    slots = tiles.shape[0]
    depth = 2 * features
    vmem = pl.BlockSpec(memory_space=pltpu.VMEM)
    pairs = clusters * slot_list.shape[1]
    return pl.pallas_call(
        sweep_kernel,
        out_shape=(
            jax.ShapeDtypeStruct((clusters, points), jnp.float32),
            jax.ShapeDtypeStruct((slots, points), jnp.float32),
        ),
        in_specs=[pl.BlockSpec(memory_space=pltpu.SMEM), vmem, vmem, vmem, vmem],
        out_specs=(vmem, vmem),
        scratch_shapes=[
            pltpu.VMEM((slots, points, depth), jnp.bfloat16),
            pltpu.VMEM((slots, depth, points), jnp.bfloat16),
            pltpu.VMEM((slots, 8, points), jnp.float32),
            pltpu.VMEM((slots, 8, points), jnp.float32),
        ],
        cost_estimate=pl.CostEstimate(
            flops=4 * pairs * points * points * depth,
            transcendentals=2 * pairs * points * points,
            bytes_accessed=2 * slots * features * points,
        ),
        name="sweep",
    )(slot_list, source, mass, tiles, u)


def place():
    rows, columns = lax.axis_size("row"), lax.axis_size("col")
    return lax.axis_index("row") * columns + lax.axis_index("col"), rows * columns, columns


def peer_of(step):
    me, devices, columns = place()
    peer = lax.rem(me + step, devices)
    return peer, (lax.div(peer, columns), lax.rem(peer, columns))


def greet():
    devices = place()[1]
    barrier = pltpu.get_barrier_semaphore()

    def signal(step, carry):
        pl.semaphore_signal(barrier, inc=1, device_id=peer_of(step)[1], device_id_type=MESH)
        return carry

    lax.fori_loop(1, devices, signal, 0)
    pl.semaphore_wait(barrier, devices - 1)


def send_all(sources, targets, send_sem, recv_sem, first):
    me, devices, _ = place()

    def send(step, carry):
        peer, where = peer_of(step)
        for index, (source, target) in enumerate(zip(sources, targets)):
            pltpu.make_async_remote_copy(
                src_ref=source.at[peer],
                dst_ref=target.at[me],
                send_sem=send_sem.at[first + index],
                recv_sem=recv_sem.at[first + index],
                device_id=where,
                device_id_type=MESH,
            ).start()
        return carry

    lax.fori_loop(1, devices, send, 0)
    for source, target in zip(sources, targets):
        target[me] = source[me]


def wait_all(refs, sems, first):
    devices = place()[1]
    for index, ref in enumerate(refs):
        blocks = ref.at[pl.ds(0, devices - 1)]
        pltpu.make_async_copy(blocks, blocks, sems.at[first + index]).wait()


def exchange_kernel(count, *refs):
    sources, targets = refs[:count], refs[count : 2 * count]
    send_sem, recv_sem = refs[2 * count :]
    greet()
    send_all(sources, targets, send_sem, recv_sem, 0)
    wait_all(targets, recv_sem, 0)
    wait_all(sources, send_sem, 0)


def exchange(arrays, collective_id):
    count = len(arrays)
    vmem = pl.BlockSpec(memory_space=pltpu.VMEM)
    return pl.pallas_call(
        functools.partial(exchange_kernel, count),
        out_shape=tuple(jax.ShapeDtypeStruct(array.shape, array.dtype) for array in arrays),
        in_specs=[vmem] * count,
        out_specs=(vmem,) * count,
        scratch_shapes=[pltpu.SemaphoreType.DMA((count,)), pltpu.SemaphoreType.DMA((count,))],
        compiler_params=pltpu.CompilerParams(collective_id=collective_id, has_side_effects=True),
        name="exchange" + str(collective_id),
    )(*arrays)


def combined(asked, parts, cluster):
    masked = jnp.where(asked == cluster, parts, lowest)
    upper = jnp.max(jnp.max(masked, axis=0), axis=0, keepdims=True)
    total = jnp.sum(jnp.sum(jnp.exp(masked - upper[None]), axis=0), axis=0, keepdims=True)
    return upper + jnp.log(total)


def turn_kernel(column_ref, asked_ref, mass_ref, u_ref, parts_ref, outgoing_ref, send_sem, recv_sem):
    greet()
    send_all([column_ref], [parts_ref], send_sem, recv_sem, 0)
    wait_all([parts_ref], recv_sem, 0)
    asked, parts = asked_ref[...], parts_ref[...]

    outgoing = jnp.zeros(parts.shape, jnp.float32)
    for cluster in range(mass_ref.shape[0]):
        row = mass_ref[cluster : cluster + 1, :] - combined(asked, parts, cluster)
        outgoing = jnp.where(asked == cluster, row[None], outgoing)
    outgoing_ref[...] = outgoing
    send_all([outgoing_ref], [u_ref], send_sem, recv_sem, 1)
    wait_all([u_ref], recv_sem, 1)
    wait_all([column_ref, outgoing_ref], send_sem, 0)


def finish_kernel(column_ref, asked_ref, level_ref, parts_ref, send_sem, recv_sem):
    greet()
    send_all([column_ref], [parts_ref], send_sem, recv_sem, 0)
    wait_all([parts_ref], recv_sem, 0)
    asked, parts = asked_ref[...], parts_ref[...]
    for cluster in range(level_ref.shape[0]):
        level_ref[cluster : cluster + 1, :] = combined(asked, parts, cluster)
    wait_all([column_ref], send_sem, 0)


def owner_call(kernel, out, scratch, collective_id, *operands):
    vmem = pl.BlockSpec(memory_space=pltpu.VMEM)
    return pl.pallas_call(
        kernel,
        out_shape=out,
        in_specs=[vmem] * len(operands),
        out_specs=vmem,
        scratch_shapes=scratch
        + [pltpu.SemaphoreType.DMA((2,)), pltpu.SemaphoreType.DMA((2,))],
        compiler_params=pltpu.CompilerParams(collective_id=collective_id, has_side_effects=True),
        name="owner" + str(collective_id),
    )(*operands)


def body(source_points, target_points, source_mass, target_mass, support, coarse_potential):
    devices = lax.axis_size(AXES)
    local_count, features, points = source_points.shape
    owner = support // local_count
    within = support % local_count
    flat_owner, flat_within = owner.reshape(-1), within.reshape(-1)
    named = flat_owner[None, :] == jnp.arange(devices, dtype=jnp.int32)[:, None]
    first = jnp.min(jnp.where(named, flat_within[None, :], local_count), axis=1)
    second = jnp.max(jnp.where(named, flat_within[None, :], -1), axis=1)
    request = jnp.stack([first, second], axis=1).astype(jnp.int32)
    shape = (devices, CAP, points)
    (asked,) = exchange([jnp.broadcast_to(request[:, :, None], shape)], 0)
    first_of = jnp.sum(jnp.where(named, first[:, None], 0), axis=0).reshape(owner.shape)
    slot_list = (owner * CAP + (within > first_of).astype(jnp.int32)).astype(jnp.int32)

    target_sq = squares(target_points)
    source_sq = squares(source_points)
    u = 2.0 * (coarse_potential - target_sq) + target_mass
    matches = asked[:, :, None, :] == jnp.arange(local_count, dtype=jnp.int32)[:, None]
    sending = jnp.sum(jnp.where(matches, u, 0.0), axis=2)
    tiles, received = exchange([target_points[asked[:, :, 0]], sending], 1)
    tiles = tiles.reshape(devices * CAP, features, points)
    row_shape = jax.ShapeDtypeStruct(shape, jnp.float32)
    level_shape = jax.ShapeDtypeStruct(target_mass.shape, jnp.float32)
    buffer = pltpu.VMEM(shape, jnp.float32)
    for sweep in range(ITERS):
        level, column = sweep_call(
            slot_list, source_points, source_mass, tiles, received.reshape(devices * CAP, points)
        )
        column = column.reshape(shape)
        if sweep < ITERS - 1:
            received = owner_call(
                turn_kernel, row_shape, [buffer, buffer], 2 + sweep, column, asked, target_mass
            )
    column_level = owner_call(finish_kernel, level_shape, [buffer], 1 + ITERS, column, asked)
    return (source_sq - 0.5 * level, target_sq - 0.5 * column_level)


def solution(mesh):
    placed = (
        P(AXES, None, None),
        P(AXES, None, None),
        P(AXES, None),
        P(AXES, None),
        P(AXES, None),
        P(AXES, None),
    )
    return jax.shard_map(
        body,
        mesh=mesh,
        in_specs=placed,
        out_specs=(P(AXES, None), P(AXES, None)),
        check_vma=False,
    )
```
